32 devices in a mesh: groups: 2 (over x), freq: 16 (over z, y, core).
Axes of the slice: x: 2, y: 2, z: 4, core: 2. Of those that a mesh axis runs over, the one named last changes fastest.
Arguments:
- traces: bfloat16 [1024, 2048, 32], P('freq', None, 'groups'), parts along dimension 2, may hold values from -6 to 6
- freq_index: int32 [16], replicated, may hold values from 1 to 511
- block_map: int32 [64, 64], replicated, may hold values 0 or 1
- green_rec: bfloat16 [16, 2, 2048, 1536], P('freq', None, None, 'groups'), parts along dimension 3, may hold values from -0.1875 to 0.1875
- green_src: bfloat16 [16, 2, 16, 1536], P('freq', None, None, 'groups'), parts along dimension 3, may hold values from -0.25 to 0.25
Outputs:
- image: float32 [1536], P(('groups', 'freq')), parts along dimension 0
The draws below stay inside these ranges and needn't reach their ends.
There are 2 independent parts, one for each index of `groups`. The reference program is written for one: setup_inputs(seed, part) draws one part's arguments, and reference() takes and returns one part's arrays. A program takes and returns all parts, laid end to end along the dimension named above; an argument that names none is the same for every part. Nothing has to cross between parts.
Inputs may be any that keep to these rules, and one draw needn't show every extreme that they name: `freq_index`: frequency bins; they may repeat. `block_map`: 1 where a receiver block lies in an image tile's aperture.
All inputs are finite; a program needn't handle non-finite values.
Results may differ from the reference program's by a relative error of at most 0.0038.
Values may be sent and summed in bfloat16 or wider, within the bound.
No kernel may reach another device: no remote copies, remote signals or barrier semaphores. Data moves between devices by JAX's collectives and lax.ppermute only.
A program may use at most 64 MiB of HBM per device.

```python
import math
import jax
import jax.numpy as jnp
from jax import lax

NT = 1024
R = 2048
RBLK = 64
TILES = 64
P_SIZE = 768
S = 16
FREQS = 16


def place_ends(result, key, low, largest):
    extent = result.shape
    spot = [jax.random.randint(jax.random.fold_in(key, axis), (), 0, extent[axis]) for axis in range(len(extent))]
    result = result.at[tuple(spot)].set(low)
    longest = extent.index(max(extent))
    spot[longest] = (spot[longest] + 1) % extent[longest]
    return result.at[tuple(spot)].set(largest)


def strengthened(entries, stream_key, source, target, shards_of, factor):
    owner, partner = [(jnp.arange(entries.shape[axis_at]) // (entries.shape[axis_at] // shards_of)).reshape([-1 if axis == axis_at else 1 for axis in range(entries.ndim)]) for axis_at in (source, target)]
    chosen = jax.random.permutation(stream_key, shards_of)[partner]
    strong = (owner == chosen) | (owner == (partner + shards_of // 2) % shards_of)
    return jnp.where(strong, factor * entries, entries)


def block_levels(key, shape, split, smallest, top_value):
    def one(position, blocks):
        heights = jax.random.uniform(jax.random.fold_in(jax.random.fold_in(key, 6), position), (blocks,), jnp.float32, smallest / len(split), top_value / len(split))
        return jnp.repeat(jnp.exp(heights), shape[position] // blocks).reshape((-1,) + (1,) * (len(shape) - position - 1))

    gain = one(*split[0])
    for cut in split[1:]:
        gain = gain * one(*cut)
    return gain


def centred(key, dims, width, bound, pieces=(), held_as=jnp.bfloat16):
    array = jax.random.normal(key, dims, jnp.float32) * width
    if len(pieces) > 0:
        array = block_levels(key, dims, pieces, -0.22, 0.18) * array
    return jnp.clip(array, min=-bound, max=bound).astype(held_as)


def gaussian_with(rng, extent, width, most, shards, heavy, kind=jnp.bfloat16):
    entries = width * jax.random.normal(rng, extent, jnp.float32)
    if shards:
        entries = entries * block_levels(rng, extent, shards, -0.22, 0.18)
    return jnp.clip(strengthened(entries, jax.random.fold_in(rng, 3), *heavy), -most, most).astype(kind)


def setup_inputs(seed: int = 0, part: int = 0) -> dict:
    key_of = jax.random.split(jax.random.key(seed), 6)
    part_keys = jax.random.split(jax.random.fold_in(key_of[5], part), 6)
    return {
        "traces": gaussian_with(part_keys[0], (NT, R, S), 1.0, 6.0, ((0, 16),), (0, 1, 16, 2.0)),
        "freq_index": place_ends(jax.random.randint(key_of[1], (FREQS,), 1, NT // 2), jax.random.fold_in(key_of[1], 1), 1, (NT // 2) - 1).astype(jnp.int32),
        "block_map": place_ends((jax.random.randint(key_of[2], (RBLK, TILES), 0, 3) < 1).astype(jnp.int32), jax.random.fold_in(key_of[2], 1), 0, 1),
        "green_rec": gaussian_with(part_keys[3], (FREQS, 2, R, P_SIZE), R ** -0.5, 0.1875, ((0, 16),), (0, 3, 16, 2.0)),
        "green_src": centred(part_keys[4], (FREQS, 2, S, P_SIZE), (2 * S * FREQS) ** -0.5, 0.25, ((0, 16),)),
    }


def dft_table(freq_index, length):
    sample_index = jnp.arange(length, dtype=jnp.int32)
    phases = freq_index[:, None] * sample_index[None, :] % length
    angles = phases.astype(jnp.float32) * jnp.float32(2.0 * math.pi / length)
    stacked = jnp.stack((jnp.cos(angles), -jnp.sin(angles)), axis=1)
    return stacked.reshape(freq_index.shape[0] * 2, length).astype(jnp.bfloat16)

def expand_map(block_map, receivers, points):
    row_span = receivers // block_map.shape[0]
    col_span = points // block_map.shape[1]
    return jnp.repeat(jnp.repeat(block_map, row_span, axis=0), col_span, axis=1).astype(jnp.bfloat16)

def reference(traces, freq_index, block_map, green_rec, green_src):
    cos_table = dft_table(freq_index, NT)
    spectrum = jnp.dot(cos_table, traces.reshape(NT, R * S), preferred_element_type=jnp.float32)
    spectrum = (spectrum * (1.0 / math.sqrt(NT))).astype(jnp.bfloat16).reshape(FREQS, 2, R, S)
    mask_full = expand_map(block_map, R, P_SIZE)

    def per_freq(image_sum, stacked):
        spec_f, rec_f, src_f = stacked
        masked = (rec_f * mask_full[None]).astype(jnp.float32)
        spec_w = spec_f.astype(jnp.float32)
        swapped = jnp.stack((spec_w[1], -spec_w[0]), axis=0)
        blocks = jnp.stack((spec_w, swapped), axis=0)
        back_field = jnp.einsum('crx,ocrs->osx', masked, blocks, precision=lax.Precision.HIGHEST)
        image_sum = image_sum + lax.optimization_barrier(jnp.sum(src_f.astype(jnp.float32) * back_field, axis=(0, 1)))
        return (image_sum, None)
    image, _ = lax.scan(per_freq, jnp.zeros((P_SIZE,), jnp.float32), (spectrum, green_rec, green_src))
    return image
```

```python
import math

import jax
import jax.numpy as jnp
from jax import lax
from jax.sharding import PartitionSpec as P


def dft_table(freq_index, length):
    sample_index = jnp.arange(length, dtype=jnp.int32)
    phases = freq_index[:, None] * sample_index[None, :] % length
    angles = phases.astype(jnp.float32) * jnp.float32(2.0 * math.pi / length)
    stacked = jnp.stack((jnp.cos(angles), -jnp.sin(angles)), axis=1)
    return stacked.reshape(freq_index.shape[0] * 2, length).astype(jnp.bfloat16)


def expand_map(block_map, receivers, points):
    row_span = receivers // block_map.shape[0]
    col_span = points // block_map.shape[1]
    return jnp.repeat(jnp.repeat(block_map, row_span, axis=0), col_span, axis=1).astype(
        jnp.bfloat16
    )


def transform(cos_table, records, length):
    spectrum = jnp.dot(cos_table, records.reshape(length, -1), preferred_element_type=jnp.float32)
    return (spectrum * (1.0 / math.sqrt(length))).astype(jnp.bfloat16)


def back_project(spectra, masked):
    swapped = jnp.stack((spectra[:, 1], -spectra[:, 0]), axis=1)
    blocks = jnp.stack((spectra, swapped), axis=1)
    return jnp.einsum("fcrx,focrs->fosx", masked, blocks, preferred_element_type=jnp.float32)


def regrouped_body(traces, freq_index, block_map, green_rec, green_src):
    shards = lax.axis_size("freq")
    length = traces.shape[0] * shards
    receivers = traces.shape[1]
    shots = traces.shape[2]
    freqs = freq_index.shape[0]
    cos_table = dft_table(freq_index, length)
    masked = green_rec * expand_map(block_map, receivers, green_rec.shape[3])[None, None]
    regrouped = lax.all_to_all(traces, "freq", split_axis=2, concat_axis=0, tiled=True)
    spectrum = transform(cos_table, regrouped, length).reshape(freqs, 2, receivers, shots // shards)
    gathered = lax.all_to_all(spectrum, "freq", split_axis=0, concat_axis=3, tiled=True)
    back_field = back_project(gathered, masked)
    partial_image = jnp.sum(green_src.astype(jnp.float32) * back_field, axis=(0, 1, 2))
    return lax.psum_scatter(partial_image, "freq", scatter_dimension=0, tiled=True)


def local_table(freq_index, length, span, position):
    chips = freq_index.shape[0] // 2
    offsets = jnp.arange(chips, dtype=jnp.int32)
    owners = jnp.concatenate(
        [2 * ((position // 2) ^ offsets) + (position % 2 ^ half) for half in range(2)]
    )
    bins = jnp.sum(
        jnp.where(owners[:, None] == jnp.arange(freq_index.shape[0])[None, :], freq_index[None, :], 0),
        axis=1,
    )
    times = position * span + jnp.arange(span, dtype=jnp.int32)
    phases = bins[:, None] * times[None, :] % length
    angles = phases.astype(jnp.float32) * jnp.float32(2.0 * math.pi / length)
    stacked = jnp.stack((jnp.cos(angles), -jnp.sin(angles)), axis=1)
    return stacked.reshape(-1, span).astype(jnp.bfloat16)


def spread_over_shots(table, shots):
    channels, span = table.shape
    rows = jnp.arange(channels * shots, dtype=jnp.int32)
    cols = jnp.arange(span * shots, dtype=jnp.int32)
    row_pick = (rows[:, None] // shots == jnp.arange(channels)[None, :]).astype(jnp.bfloat16)
    col_pick = (cols[None, :] // shots == jnp.arange(span)[:, None]).astype(jnp.bfloat16)
    tall = jnp.dot(row_pick, table, preferred_element_type=jnp.bfloat16)
    wide = jnp.dot(tall, col_pick, preferred_element_type=jnp.bfloat16)
    return jnp.where(rows[:, None] % shots == cols[None, :] % shots, wide, jnp.bfloat16(0))


def partial_body(traces, freq_index, block_map, green_rec, green_src):
    shards = lax.axis_size("freq")
    chips = shards // 2
    span, receivers, shots = traces.shape
    points = green_rec.shape[3]
    length = span * shards
    position = lax.axis_index("freq")
    masked = green_rec * expand_map(block_map, receivers, points)[None, None]

    records = traces.transpose(0, 2, 1).reshape(span * shots, receivers)
    table = spread_over_shots(local_table(freq_index, length, span, position), shots)
    partial = jnp.dot(table, records, preferred_element_type=jnp.float32)
    partial = partial.reshape(2, chips, 2 * shots, receivers)
    sibling = [(j, j ^ 1) for j in range(shards)]
    received = lax.ppermute(partial[1].astype(jnp.bfloat16), "freq", sibling)
    paired = partial[0] + received.astype(jnp.float32)
    total = paired[0]
    arrived = [
        lax.ppermute(
            paired[k].astype(jnp.bfloat16),
            "freq",
            [(j, j ^ (2 * k)) for j in range(shards)],
        )
        for k in range(1, chips)
    ]
    for piece in arrived:
        total = total + piece.astype(jnp.float32)
    spectrum = (total * (1.0 / math.sqrt(length))).astype(jnp.bfloat16)
    swapped = jnp.concatenate((spectrum[shots:], -spectrum[:shots]), axis=0)
    back = jnp.dot(spectrum, masked[0, 0], preferred_element_type=jnp.float32)
    back = back + jnp.dot(swapped, masked[0, 1], preferred_element_type=jnp.float32)
    weights = green_src.astype(jnp.float32).reshape(2 * shots, points)
    image = jnp.sum(weights * back, axis=0)
    pieces = lax.all_to_all(
        image.reshape(shards, points // shards), "freq", split_axis=0, concat_axis=0, tiled=True
    )
    return jnp.sum(pieces, axis=0)


def body(traces, freq_index, block_map, green_rec, green_src):
    shards = lax.axis_size("freq")
    freqs = freq_index.shape[0]
    paired_chips = shards % 2 == 0 and shards & (shards - 1) == 0
    if freqs == shards and paired_chips and 2 * freqs <= traces.shape[0]:
        return partial_body(traces, freq_index, block_map, green_rec, green_src)
    return regrouped_body(traces, freq_index, block_map, green_rec, green_src)


def solution(mesh):
    in_specs = (
        P("freq", None, "groups"),
        P(),
        P(),
        P("freq", None, None, "groups"),
        P("freq", None, None, "groups"),
    )
    out_specs = P(("groups", "freq"))
    return jax.shard_map(body, mesh=mesh, in_specs=in_specs, out_specs=out_specs, check_vma=False)
```

```python
import functools
import math

import jax
import jax.numpy as jnp
from jax import lax
from jax.experimental import pallas as pl
from jax.experimental.pallas import tpu as pltpu
from jax.sharding import PartitionSpec as P


def dft_table(freq_index, length):
    sample_index = jnp.arange(length, dtype=jnp.int32)
    phases = freq_index[:, None] * sample_index[None, :] % length
    angles = phases.astype(jnp.float32) * jnp.float32(2.0 * math.pi / length)
    stacked = jnp.stack((jnp.cos(angles), -jnp.sin(angles)), axis=1)
    return stacked.reshape(freq_index.shape[0] * 2, length).astype(jnp.bfloat16)


def expand_map(block_map, receivers, points):
    row_span = receivers // block_map.shape[0]
    col_span = points // block_map.shape[1]
    return jnp.repeat(jnp.repeat(block_map, row_span, axis=0), col_span, axis=1).astype(
        jnp.bfloat16
    )


def transform(cos_table, records, length):
    spectrum = jnp.dot(cos_table, records.reshape(length, -1), preferred_element_type=jnp.float32)
    return (spectrum * (1.0 / math.sqrt(length))).astype(jnp.bfloat16)


def back_project(spectra, masked):
    swapped = jnp.stack((spectra[:, 1], -spectra[:, 0]), axis=1)
    blocks = jnp.stack((spectra, swapped), axis=1)
    return jnp.einsum("fcrx,focrs->fosx", masked, blocks, preferred_element_type=jnp.float32)


def regrouped_body(traces, freq_index, block_map, green_rec, green_src):
    shards = lax.axis_size("freq")
    length = traces.shape[0] * shards
    receivers = traces.shape[1]
    shots = traces.shape[2]
    freqs = freq_index.shape[0]
    cos_table = dft_table(freq_index, length)
    masked = green_rec * expand_map(block_map, receivers, green_rec.shape[3])[None, None]
    regrouped = lax.all_to_all(traces, "freq", split_axis=2, concat_axis=0, tiled=True)
    spectrum = transform(cos_table, regrouped, length).reshape(freqs, 2, receivers, shots // shards)
    gathered = lax.all_to_all(spectrum, "freq", split_axis=0, concat_axis=3, tiled=True)
    back_field = back_project(gathered, masked)
    partial_image = jnp.sum(green_src.astype(jnp.float32) * back_field, axis=(0, 1, 2))
    return lax.psum_scatter(partial_image, "freq", scatter_dimension=0, tiled=True)


def local_table(freq_index, length, span, position):
    times = position * span + jnp.arange(span, dtype=jnp.int32)
    phases = freq_index[:, None] * times[None, :] % length
    angles = phases.astype(jnp.float32) * jnp.float32(2.0 * math.pi / length)
    stacked = jnp.stack((jnp.cos(angles), -jnp.sin(angles)), axis=1)
    return stacked.reshape(-1, span).astype(jnp.bfloat16)


def transform_kernel(position_ref, table_ref, records_ref, keep_ref, send_ref, spread_ref, *, shots):
    channels, span = table_ref.shape
    rows, cols = spread_ref.shape

    @pl.when(pl.program_id(0) == 0)
    def _():
        position = position_ref[0]
        chip = position // 2
        core = position % 2
        row = lax.broadcasted_iota(jnp.int32, (rows, channels), 0)
        channel = row // shots
        half = channel // (channels // 2)
        slot = channel % (channels // 2)
        source = 2 * (2 * ((slot // 2) ^ chip) + (half ^ core)) + slot % 2
        wanted = lax.broadcasted_iota(jnp.int32, (rows, channels), 1)
        row_pick = jnp.where(source == wanted, 1.0, 0.0).astype(jnp.bfloat16)
        tall = jnp.dot(row_pick, table_ref[...], preferred_element_type=jnp.float32)
        time = lax.broadcasted_iota(jnp.int32, (span, cols), 0)
        col = lax.broadcasted_iota(jnp.int32, (span, cols), 1)
        col_pick = jnp.where(col // shots == time, 1.0, 0.0).astype(jnp.bfloat16)
        wide = jnp.dot(tall.astype(jnp.bfloat16), col_pick, preferred_element_type=jnp.float32)
        row_shot = lax.broadcasted_iota(jnp.int32, (rows, cols), 0) % shots
        col_shot = lax.broadcasted_iota(jnp.int32, (rows, cols), 1) % shots
        spread_ref[...] = jnp.where(row_shot == col_shot, wide, 0.0).astype(jnp.bfloat16)

    result = jnp.dot(spread_ref[...], records_ref[...], preferred_element_type=jnp.float32)
    keep_ref[...] = result[: rows // 2]
    send_ref[...] = result[rows // 2 :].astype(jnp.bfloat16)


def transform_own_samples(table, records, position, shots):
    channels, span = table.shape
    receivers = records.shape[1]
    rows, cols = channels * shots, span * shots
    block = min(512, receivers)
    return pl.pallas_call(
        functools.partial(transform_kernel, shots=shots),
        grid=(receivers // block,),
        in_specs=[
            pl.BlockSpec(memory_space=pltpu.SMEM),
            pl.BlockSpec((channels, span), lambda i: (0, 0)),
            pl.BlockSpec((cols, block), lambda i: (0, i)),
        ],
        out_specs=[
            pl.BlockSpec((rows // 2, block), lambda i: (0, i)),
            pl.BlockSpec((rows // 2, block), lambda i: (0, i)),
        ],
        out_shape=[
            jax.ShapeDtypeStruct((rows // 2, receivers), jnp.float32),
            jax.ShapeDtypeStruct((rows // 2, receivers), jnp.bfloat16),
        ],
        scratch_shapes=[pltpu.VMEM((rows, cols), jnp.bfloat16)],
        name="transform_own_samples",
    )(position.reshape(1), table, records)


def mask_green(green_rec, block_map):
    parts, receivers, points = green_rec.shape
    row_blocks, tiles = block_map.shape
    col_span = points // tiles
    col_pick = (jnp.arange(points)[None, :] // col_span == jnp.arange(tiles)[:, None]).astype(jnp.bfloat16)
    columns = jnp.dot(block_map.astype(jnp.bfloat16), col_pick, preferred_element_type=jnp.bfloat16)
    split = green_rec.reshape(parts, row_blocks, receivers // row_blocks, points)
    return (split * columns[None, :, None, :]).reshape(parts, receivers, points)


def far_first(chips):
    return sorted(range(1, chips), key=lambda k: (-(k // 2), k % 2))


def partial_body(traces, freq_index, block_map, green_rec, green_src):
    shards = lax.axis_size("freq")
    chips = shards // 2
    span, receivers, shots = traces.shape
    points = green_rec.shape[3]
    length = span * shards
    position = lax.axis_index("freq")

    records = traces.transpose(0, 2, 1).reshape(span * shots, receivers)
    table = local_table(freq_index, length, span, position)
    keep, send = transform_own_samples(table, records, position, shots)
    received = lax.ppermute(send, "freq", [(j, j ^ 1) for j in range(shards)])
    paired = (keep + received.astype(jnp.float32)).reshape(chips, 2 * shots, receivers)
    paired, late_map = lax.optimization_barrier((paired, block_map))
    total = paired[0]
    arrived = [
        lax.ppermute(
            paired[k].astype(jnp.bfloat16),
            "freq",
            [(j, j ^ (2 * k)) for j in range(shards)],
        )
        for k in far_first(chips)
    ]
    masked = mask_green(green_rec[0], late_map)
    for piece in arrived:
        total = total + piece.astype(jnp.float32)
    spectrum = (total * (1.0 / math.sqrt(length))).astype(jnp.bfloat16)
    swapped = jnp.concatenate((spectrum[shots:], -spectrum[:shots]), axis=0)
    back = jnp.dot(spectrum, masked[0], preferred_element_type=jnp.float32)
    back = back + jnp.dot(swapped, masked[1], preferred_element_type=jnp.float32)
    weights = green_src.astype(jnp.float32).reshape(2 * shots, points)
    image = jnp.sum(weights * back, axis=0)
    pieces = lax.all_to_all(
        image.reshape(shards, points // shards), "freq", split_axis=0, concat_axis=0, tiled=True
    )
    return jnp.sum(pieces, axis=0)


def body(traces, freq_index, block_map, green_rec, green_src):
    shards = lax.axis_size("freq")
    freqs = freq_index.shape[0]
    paired_chips = shards % 2 == 0 and shards & (shards - 1) == 0
    if freqs == shards and paired_chips and 2 * freqs <= traces.shape[0]:
        return partial_body(traces, freq_index, block_map, green_rec, green_src)
    return regrouped_body(traces, freq_index, block_map, green_rec, green_src)


def solution(mesh):
    in_specs = (
        P("freq", None, "groups"),
        P(),
        P(),
        P("freq", None, None, "groups"),
        P("freq", None, None, "groups"),
    )
    out_specs = P(("groups", "freq"))
    return jax.shard_map(body, mesh=mesh, in_specs=in_specs, out_specs=out_specs, check_vma=False)
```

```python
import functools
import math

import jax
import jax.numpy as jnp
from jax import lax
from jax.experimental import pallas as pl
from jax.experimental.pallas import tpu as pltpu
from jax.sharding import PartitionSpec as P


def dft_table(freq_index, length):
    sample_index = jnp.arange(length, dtype=jnp.int32)
    phases = freq_index[:, None] * sample_index[None, :] % length
    angles = phases.astype(jnp.float32) * jnp.float32(2.0 * math.pi / length)
    stacked = jnp.stack((jnp.cos(angles), -jnp.sin(angles)), axis=1)
    return stacked.reshape(freq_index.shape[0] * 2, length).astype(jnp.bfloat16)


def expand_map(block_map, receivers, points):
    row_span = receivers // block_map.shape[0]
    col_span = points // block_map.shape[1]
    return jnp.repeat(jnp.repeat(block_map, row_span, axis=0), col_span, axis=1).astype(
        jnp.bfloat16
    )


def transform(cos_table, records, length):
    spectrum = jnp.dot(cos_table, records.reshape(length, -1), preferred_element_type=jnp.float32)
    return (spectrum * (1.0 / math.sqrt(length))).astype(jnp.bfloat16)


def back_project(spectra, masked):
    swapped = jnp.stack((spectra[:, 1], -spectra[:, 0]), axis=1)
    blocks = jnp.stack((spectra, swapped), axis=1)
    return jnp.einsum("fcrx,focrs->fosx", masked, blocks, preferred_element_type=jnp.float32)


def regrouped_body(traces, freq_index, block_map, green_rec, green_src):
    shards = lax.axis_size("freq")
    length = traces.shape[0] * shards
    receivers = traces.shape[1]
    shots = traces.shape[2]
    freqs = freq_index.shape[0]
    cos_table = dft_table(freq_index, length)
    masked = green_rec * expand_map(block_map, receivers, green_rec.shape[3])[None, None]
    regrouped = lax.all_to_all(traces, "freq", split_axis=2, concat_axis=0, tiled=True)
    spectrum = transform(cos_table, regrouped, length).reshape(freqs, 2, receivers, shots // shards)
    gathered = lax.all_to_all(spectrum, "freq", split_axis=0, concat_axis=3, tiled=True)
    back_field = back_project(gathered, masked)
    partial_image = jnp.sum(green_src.astype(jnp.float32) * back_field, axis=(0, 1, 2))
    return lax.psum_scatter(partial_image, "freq", scatter_dimension=0, tiled=True)


def local_table(freq_index, length, span, position):
    times = position * span + jnp.arange(span, dtype=jnp.int32)
    phases = freq_index[:, None] * times[None, :] % length
    angles = phases.astype(jnp.float32) * jnp.float32(2.0 * math.pi / length)
    return jnp.cos(angles).astype(jnp.bfloat16), (-jnp.sin(angles)).astype(jnp.bfloat16)


def transform_kernel(
    position_ref, real_ref, imag_ref, records_ref, keep_ref, send_ref, spread_ref, *, shots, slots
):
    freqs, span = real_ref.shape
    rows, cols = spread_ref.shape

    @pl.when(pl.program_id(0) == 0)
    def _():
        position = position_ref[0]
        chip = position // 2
        core = position % 2
        channel = lax.broadcasted_iota(jnp.int32, (rows, freqs), 0) // shots
        half = channel // (2 * len(slots))
        group = channel // 2 % len(slots)
        slot = sum(jnp.where(group == i, slots[i], 0) for i in range(len(slots)))
        source = 2 * (slot ^ chip) + (half ^ core)
        wanted = source == lax.broadcasted_iota(jnp.int32, (rows, freqs), 1)
        real_pick = jnp.where(wanted & (channel % 2 == 0), 1.0, 0.0).astype(jnp.bfloat16)
        imag_pick = jnp.where(wanted & (channel % 2 == 1), 1.0, 0.0).astype(jnp.bfloat16)
        tall = jnp.dot(real_pick, real_ref[...], preferred_element_type=jnp.float32)
        tall = tall + jnp.dot(imag_pick, imag_ref[...], preferred_element_type=jnp.float32)
        time = lax.broadcasted_iota(jnp.int32, (span, cols), 0)
        col = lax.broadcasted_iota(jnp.int32, (span, cols), 1)
        col_pick = jnp.where(col // shots == time, 1.0, 0.0).astype(jnp.bfloat16)
        wide = jnp.dot(tall.astype(jnp.bfloat16), col_pick, preferred_element_type=jnp.float32)
        row_shot = lax.broadcasted_iota(jnp.int32, (rows, 1), 0) % shots
        col_shot = lax.broadcasted_iota(jnp.int32, (1, cols), 1) % shots
        spread_ref[...] = jnp.where(row_shot == col_shot, wide, 0.0).astype(jnp.bfloat16)

    result = jnp.dot(spread_ref[...], records_ref[...], preferred_element_type=jnp.float32)
    keep_ref[...] = result[: rows // 2]
    send_ref[...] = result[rows // 2 :].astype(jnp.bfloat16)


def transform_own_samples(table, records, position, shots, slots):
    freqs, span = table[0].shape
    receivers = records.shape[1]
    rows, cols = 4 * len(slots) * shots, span * shots
    block = min(512, receivers)
    return pl.pallas_call(
        functools.partial(transform_kernel, shots=shots, slots=slots),
        grid=(receivers // block,),
        in_specs=[
            pl.BlockSpec(memory_space=pltpu.SMEM),
            pl.BlockSpec((freqs, span), lambda i: (0, 0)),
            pl.BlockSpec((freqs, span), lambda i: (0, 0)),
            pl.BlockSpec((cols, block), lambda i: (0, i)),
        ],
        out_specs=[
            pl.BlockSpec((rows // 2, block), lambda i: (0, i)),
            pl.BlockSpec((rows // 2, block), lambda i: (0, i)),
        ],
        out_shape=[
            jax.ShapeDtypeStruct((rows // 2, receivers), jnp.float32),
            jax.ShapeDtypeStruct((rows // 2, receivers), jnp.bfloat16),
        ],
        scratch_shapes=[pltpu.VMEM((rows, cols), jnp.bfloat16)],
        name="transform_own_samples",
    )(position.reshape(1), *table, records)


def mask_green(green_rec, block_map):
    parts, receivers, points = green_rec.shape
    row_blocks, tiles = block_map.shape
    col_span = points // tiles
    col_pick = (jnp.arange(points)[None, :] // col_span == jnp.arange(tiles)[:, None]).astype(jnp.bfloat16)
    columns = jnp.dot(block_map.astype(jnp.bfloat16), col_pick, preferred_element_type=jnp.bfloat16)
    split = green_rec.reshape(parts, row_blocks, receivers // row_blocks, points)
    return (split * columns[None, :, None, :]).reshape(parts, receivers, points)


def partial_body(traces, freq_index, block_map, green_rec, green_src):
    shards = lax.axis_size("freq")
    chips = shards // 2
    span, receivers, shots = traces.shape
    points = green_rec.shape[3]
    length = span * shards
    position = lax.axis_index("freq")
    records = traces.transpose(0, 2, 1).reshape(span * shots, receivers)
    table = local_table(freq_index, length, span, position)

    def across(array, offset):
        return lax.ppermute(array, "freq", [(j, j ^ offset) for j in range(shards)])

    def chip_sums(data, slots):
        keep, send = transform_own_samples(table, data, position, shots, slots)
        received = across(send, 1)
        return (keep + received.astype(jnp.float32)).reshape(len(slots), 2 * shots, receivers)

    far_even = tuple(range(chips // 2, chips, 2))
    far_odd = tuple(k ^ 1 for k in far_even)
    near = tuple(range(chips // 2))

    far = chip_sums(records, far_even + far_odd)
    far, late_records = lax.optimization_barrier((far, records))
    beside = across(far[len(far_even) :].astype(jnp.bfloat16), 2)
    close = chip_sums(late_records, near)
    far_sums = far[: len(far_even)] + beside.astype(jnp.float32)
    far_sums, close, late_map = lax.optimization_barrier((far_sums, close, block_map))
    arrived = [
        across(far_sums[i].astype(jnp.bfloat16), 2 * far_even[i])
        for i in reversed(range(len(far_even)))
    ]
    arrived += [across(close[k].astype(jnp.bfloat16), 2 * k) for k in reversed(near[1:])]
    masked = mask_green(green_rec[0], late_map)
    total = close[0]
    for piece in arrived:
        total = total + piece.astype(jnp.float32)
    spectrum = (total * (1.0 / math.sqrt(length))).astype(jnp.bfloat16)
    swapped = jnp.concatenate((spectrum[shots:], -spectrum[:shots]), axis=0)
    back = jnp.dot(spectrum, masked[0], preferred_element_type=jnp.float32)
    back = back + jnp.dot(swapped, masked[1], preferred_element_type=jnp.float32)
    weights = green_src.astype(jnp.float32).reshape(2 * shots, points)
    image = jnp.sum(weights * back, axis=0)
    pieces = lax.all_to_all(
        image.reshape(shards, points // shards), "freq", split_axis=0, concat_axis=0, tiled=True
    )
    return jnp.sum(pieces, axis=0)


def body(traces, freq_index, block_map, green_rec, green_src):
    shards = lax.axis_size("freq")
    freqs = freq_index.shape[0]
    paired_chips = shards >= 8 and shards & (shards - 1) == 0
    if freqs == shards and paired_chips and 2 * freqs <= traces.shape[0]:
        return partial_body(traces, freq_index, block_map, green_rec, green_src)
    return regrouped_body(traces, freq_index, block_map, green_rec, green_src)


def solution(mesh):
    in_specs = (
        P("freq", None, "groups"),
        P(),
        P(),
        P("freq", None, None, "groups"),
        P("freq", None, None, "groups"),
    )
    out_specs = P(("groups", "freq"))
    return jax.shard_map(body, mesh=mesh, in_specs=in_specs, out_specs=out_specs, check_vma=False)
```

```python
import functools
import math

import jax
import jax.numpy as jnp
from jax import lax
from jax.experimental import pallas as pl
from jax.experimental.pallas import tpu as pltpu
from jax.sharding import PartitionSpec as P


def dft_table(freq_index, length):
    sample_index = jnp.arange(length, dtype=jnp.int32)
    phases = freq_index[:, None] * sample_index[None, :] % length
    angles = phases.astype(jnp.float32) * jnp.float32(2.0 * math.pi / length)
    stacked = jnp.stack((jnp.cos(angles), -jnp.sin(angles)), axis=1)
    return stacked.reshape(freq_index.shape[0] * 2, length).astype(jnp.bfloat16)


def expand_map(block_map, receivers, points):
    row_span = receivers // block_map.shape[0]
    col_span = points // block_map.shape[1]
    return jnp.repeat(jnp.repeat(block_map, row_span, axis=0), col_span, axis=1).astype(
        jnp.bfloat16
    )


def transform(cos_table, records, length):
    spectrum = jnp.dot(cos_table, records.reshape(length, -1), preferred_element_type=jnp.float32)
    return (spectrum * (1.0 / math.sqrt(length))).astype(jnp.bfloat16)


def back_project(spectra, masked):
    swapped = jnp.stack((spectra[:, 1], -spectra[:, 0]), axis=1)
    blocks = jnp.stack((spectra, swapped), axis=1)
    return jnp.einsum("fcrx,focrs->fosx", masked, blocks, preferred_element_type=jnp.float32)


def regrouped_body(traces, freq_index, block_map, green_rec, green_src):
    shards = lax.axis_size("freq")
    length = traces.shape[0] * shards
    receivers = traces.shape[1]
    shots = traces.shape[2]
    freqs = freq_index.shape[0]
    cos_table = dft_table(freq_index, length)
    masked = green_rec * expand_map(block_map, receivers, green_rec.shape[3])[None, None]
    regrouped = lax.all_to_all(traces, "freq", split_axis=2, concat_axis=0, tiled=True)
    spectrum = transform(cos_table, regrouped, length).reshape(freqs, 2, receivers, shots // shards)
    gathered = lax.all_to_all(spectrum, "freq", split_axis=0, concat_axis=3, tiled=True)
    back_field = back_project(gathered, masked)
    partial_image = jnp.sum(green_src.astype(jnp.float32) * back_field, axis=(0, 1, 2))
    return lax.psum_scatter(partial_image, "freq", scatter_dimension=0, tiled=True)


def local_table(freq_index, length, span, position):
    times = position * span + jnp.arange(span, dtype=jnp.int32)
    phases = freq_index[:, None] * times[None, :] % length
    angles = phases.astype(jnp.float32) * jnp.float32(2.0 * math.pi / length)
    return jnp.cos(angles).astype(jnp.bfloat16), (-jnp.sin(angles)).astype(jnp.bfloat16)


def transform_kernel(
    position_ref,
    real_ref,
    imag_ref,
    records_ref,
    far_keep_ref,
    near_keep_ref,
    far_send_ref,
    near_send_ref,
    spread_ref,
    *,
    shots,
    slots,
):
    freqs, span = real_ref.shape
    rows, cols = spread_ref.shape

    @pl.when(pl.program_id(0) == 0)
    def _():
        position = position_ref[0]
        chip = position // 2
        core = position % 2
        channel = lax.broadcasted_iota(jnp.int32, (rows, freqs), 0) // shots
        half = channel // (2 * len(slots))
        group = channel // 2 % len(slots)
        slot = sum(jnp.where(group == i, slots[i], 0) for i in range(len(slots)))
        source = 2 * (slot ^ chip) + (half ^ core)
        wanted = source == lax.broadcasted_iota(jnp.int32, (rows, freqs), 1)
        real_pick = jnp.where(wanted & (channel % 2 == 0), 1.0, 0.0).astype(jnp.bfloat16)
        imag_pick = jnp.where(wanted & (channel % 2 == 1), 1.0, 0.0).astype(jnp.bfloat16)
        tall = jnp.dot(real_pick, real_ref[...], preferred_element_type=jnp.float32)
        tall = tall + jnp.dot(imag_pick, imag_ref[...], preferred_element_type=jnp.float32)
        time = lax.broadcasted_iota(jnp.int32, (span, cols), 0)
        col = lax.broadcasted_iota(jnp.int32, (span, cols), 1)
        col_pick = jnp.where(col // shots == time, 1.0, 0.0).astype(jnp.bfloat16)
        wide = jnp.dot(tall.astype(jnp.bfloat16), col_pick, preferred_element_type=jnp.float32)
        row_shot = lax.broadcasted_iota(jnp.int32, (rows, 1), 0) % shots
        col_shot = lax.broadcasted_iota(jnp.int32, (1, cols), 1) % shots
        spread_ref[...] = jnp.where(row_shot == col_shot, wide, 0.0).astype(jnp.bfloat16)

    result = jnp.dot(spread_ref[...], records_ref[...], preferred_element_type=jnp.float32)
    quarter = rows // 4
    far_keep_ref[...] = result[:quarter]
    near_keep_ref[...] = result[quarter : 2 * quarter]
    far_send_ref[...] = result[2 * quarter : 3 * quarter].astype(jnp.bfloat16)
    near_send_ref[...] = result[3 * quarter :].astype(jnp.bfloat16)


def transform_own_samples(table, records, position, shots, slots):
    freqs, span = table[0].shape
    receivers = records.shape[1]
    rows, cols = 4 * len(slots) * shots, span * shots
    block = min(256, receivers)
    return pl.pallas_call(
        functools.partial(transform_kernel, shots=shots, slots=slots),
        grid=(receivers // block,),
        in_specs=[
            pl.BlockSpec(memory_space=pltpu.SMEM),
            pl.BlockSpec((freqs, span), lambda i: (0, 0)),
            pl.BlockSpec((freqs, span), lambda i: (0, 0)),
            pl.BlockSpec((cols, block), lambda i: (0, i)),
        ],
        out_specs=[pl.BlockSpec((rows // 4, block), lambda i: (0, i))] * 4,
        out_shape=[
            jax.ShapeDtypeStruct((rows // 4, receivers), dtype)
            for dtype in (jnp.float32, jnp.float32, jnp.bfloat16, jnp.bfloat16)
        ],
        scratch_shapes=[pltpu.VMEM((rows, cols), jnp.bfloat16)],
        name="transform_own_samples",
    )(position.reshape(1), *table, records)


def mask_green(green_rec, block_map):
    parts, receivers, points = green_rec.shape
    row_blocks, tiles = block_map.shape
    col_span = points // tiles
    col_pick = (jnp.arange(points)[None, :] // col_span == jnp.arange(tiles)[:, None]).astype(jnp.bfloat16)
    columns = jnp.dot(block_map.astype(jnp.bfloat16), col_pick, preferred_element_type=jnp.bfloat16)
    split = green_rec.reshape(parts, row_blocks, receivers // row_blocks, points)
    return (split * columns[None, :, None, :]).reshape(parts, receivers, points)


def partial_body(traces, freq_index, block_map, green_rec, green_src):
    shards = lax.axis_size("freq")
    chips = shards // 2
    span, receivers, shots = traces.shape
    points = green_rec.shape[3]
    length = span * shards
    position = lax.axis_index("freq")
    records = traces.transpose(0, 2, 1).reshape(span * shots, receivers)
    table = local_table(freq_index, length, span, position)

    def across(array, offset):
        return lax.ppermute(array, "freq", [(j, j ^ offset) for j in range(shards)])

    def chip_sums(keep, received):
        return (keep + received.astype(jnp.float32)).reshape(-1, 2 * shots, receivers)

    far = range(chips // 2, chips)
    passed = [k for k in far if k >= 3 * chips // 4 and k % 2 == 1]
    summed = [k ^ 1 for k in passed]
    straight = [k for k in reversed(far) if k < 3 * chips // 4]
    near = list(range(chips // 2))
    far_slots = passed + summed + straight

    far_keep, near_keep, far_send, near_send = transform_own_samples(
        table, records, position, shots, tuple(far_slots + near)
    )
    far_received = across(far_send, 1)
    near_received = across(near_send, 1)
    far = chip_sums(far_keep, far_received)
    cut = len(passed)
    beside = across(far[:cut].astype(jnp.bfloat16), 2)
    arrived = [
        across(far[2 * cut + i].astype(jnp.bfloat16), 2 * k) for i, k in enumerate(straight)
    ]
    far_sums = far[cut : 2 * cut] + beside.astype(jnp.float32)
    far_sums, near_received, near_keep, late_map = lax.optimization_barrier(
        (far_sums, near_received, near_keep, block_map)
    )
    arrived += [across(far_sums[i].astype(jnp.bfloat16), 2 * k) for i, k in enumerate(summed)]
    close = chip_sums(near_keep, near_received)
    arrived += [across(close[k].astype(jnp.bfloat16), 2 * k) for k in reversed(near[1:])]
    masked = mask_green(green_rec[0], late_map)
    total = close[0]
    for piece in arrived:
        total = total + piece.astype(jnp.float32)
    spectrum = (total * (1.0 / math.sqrt(length))).astype(jnp.bfloat16)
    swapped = jnp.concatenate((spectrum[shots:], -spectrum[:shots]), axis=0)
    back = jnp.dot(spectrum, masked[0], preferred_element_type=jnp.float32)
    back = back + jnp.dot(swapped, masked[1], preferred_element_type=jnp.float32)
    weights = green_src.astype(jnp.float32).reshape(2 * shots, points)
    image = jnp.sum(weights * back, axis=0)
    pieces = lax.all_to_all(
        image.reshape(shards, points // shards), "freq", split_axis=0, concat_axis=0, tiled=True
    )
    return jnp.sum(pieces, axis=0)


def body(traces, freq_index, block_map, green_rec, green_src):
    shards = lax.axis_size("freq")
    freqs = freq_index.shape[0]
    paired_chips = shards >= 8 and shards & (shards - 1) == 0
    if freqs == shards and paired_chips and 2 * freqs <= traces.shape[0]:
        return partial_body(traces, freq_index, block_map, green_rec, green_src)
    return regrouped_body(traces, freq_index, block_map, green_rec, green_src)


def solution(mesh):
    in_specs = (
        P("freq", None, "groups"),
        P(),
        P(),
        P("freq", None, None, "groups"),
        P("freq", None, None, "groups"),
    )
    out_specs = P(("groups", "freq"))
    return jax.shard_map(body, mesh=mesh, in_specs=in_specs, out_specs=out_specs, check_vma=False)
```

```python
import functools
import math

import jax
import jax.numpy as jnp
from jax import lax
from jax.experimental import pallas as pl
from jax.experimental.pallas import tpu as pltpu
from jax.sharding import PartitionSpec as P


def dft_table(freq_index, length):
    sample_index = jnp.arange(length, dtype=jnp.int32)
    phases = freq_index[:, None] * sample_index[None, :] % length
    angles = phases.astype(jnp.float32) * jnp.float32(2.0 * math.pi / length)
    stacked = jnp.stack((jnp.cos(angles), -jnp.sin(angles)), axis=1)
    return stacked.reshape(freq_index.shape[0] * 2, length).astype(jnp.bfloat16)


def expand_map(block_map, receivers, points):
    row_span = receivers // block_map.shape[0]
    col_span = points // block_map.shape[1]
    return jnp.repeat(jnp.repeat(block_map, row_span, axis=0), col_span, axis=1).astype(
        jnp.bfloat16
    )


def transform(cos_table, records, length):
    spectrum = jnp.dot(cos_table, records.reshape(length, -1), preferred_element_type=jnp.float32)
    return (spectrum * (1.0 / math.sqrt(length))).astype(jnp.bfloat16)


def back_project(spectra, masked):
    swapped = jnp.stack((spectra[:, 1], -spectra[:, 0]), axis=1)
    blocks = jnp.stack((spectra, swapped), axis=1)
    return jnp.einsum("fcrx,focrs->fosx", masked, blocks, preferred_element_type=jnp.float32)


def regrouped_body(traces, freq_index, block_map, green_rec, green_src):
    shards = lax.axis_size("freq")
    length = traces.shape[0] * shards
    receivers = traces.shape[1]
    shots = traces.shape[2]
    freqs = freq_index.shape[0]
    cos_table = dft_table(freq_index, length)
    masked = green_rec * expand_map(block_map, receivers, green_rec.shape[3])[None, None]
    regrouped = lax.all_to_all(traces, "freq", split_axis=2, concat_axis=0, tiled=True)
    spectrum = transform(cos_table, regrouped, length).reshape(freqs, 2, receivers, shots // shards)
    gathered = lax.all_to_all(spectrum, "freq", split_axis=0, concat_axis=3, tiled=True)
    back_field = back_project(gathered, masked)
    partial_image = jnp.sum(green_src.astype(jnp.float32) * back_field, axis=(0, 1, 2))
    return lax.psum_scatter(partial_image, "freq", scatter_dimension=0, tiled=True)


def local_table(freq_index, length, span, position):
    times = position * span + jnp.arange(span, dtype=jnp.int32)
    phases = freq_index[:, None] * times[None, :] % length
    angles = phases.astype(jnp.float32) * jnp.float32(2.0 * math.pi / length)
    return jnp.cos(angles).astype(jnp.bfloat16), (-jnp.sin(angles)).astype(jnp.bfloat16)


def transform_kernel(
    position_ref,
    real_ref,
    imag_ref,
    records_ref,
    far_keep_ref,
    near_keep_ref,
    far_send_ref,
    near_send_ref,
    spread_ref,
    *,
    shots,
    slots,
):
    freqs, span = real_ref.shape
    rows, cols = spread_ref.shape

    @pl.when(pl.program_id(0) == 0)
    def _():
        position = position_ref[0]
        chip = position // 2
        core = position % 2
        channel = lax.broadcasted_iota(jnp.int32, (rows, freqs), 0) // shots
        half = channel // (2 * len(slots))
        group = channel // 2 % len(slots)
        slot = sum(jnp.where(group == i, slots[i], 0) for i in range(len(slots)))
        source = 2 * (slot ^ chip) + (half ^ core)
        wanted = source == lax.broadcasted_iota(jnp.int32, (rows, freqs), 1)
        real_pick = jnp.where(wanted & (channel % 2 == 0), 1.0, 0.0).astype(jnp.bfloat16)
        imag_pick = jnp.where(wanted & (channel % 2 == 1), 1.0, 0.0).astype(jnp.bfloat16)
        tall = jnp.dot(real_pick, real_ref[...], preferred_element_type=jnp.float32)
        tall = tall + jnp.dot(imag_pick, imag_ref[...], preferred_element_type=jnp.float32)
        time = lax.broadcasted_iota(jnp.int32, (span, cols), 0)
        col = lax.broadcasted_iota(jnp.int32, (span, cols), 1)
        col_pick = jnp.where(col // shots == time, 1.0, 0.0).astype(jnp.bfloat16)
        wide = jnp.dot(tall.astype(jnp.bfloat16), col_pick, preferred_element_type=jnp.float32)
        row_shot = lax.broadcasted_iota(jnp.int32, (rows, 1), 0) % shots
        col_shot = lax.broadcasted_iota(jnp.int32, (1, cols), 1) % shots
        spread_ref[...] = jnp.where(row_shot == col_shot, wide, 0.0).astype(jnp.bfloat16)

    result = jnp.dot(spread_ref[...], records_ref[...], preferred_element_type=jnp.float32)
    quarter = rows // 4
    far_keep_ref[...] = result[:quarter]
    near_keep_ref[...] = result[quarter : 2 * quarter]
    far_send_ref[...] = result[2 * quarter : 3 * quarter].astype(jnp.bfloat16)
    near_send_ref[...] = result[3 * quarter :].astype(jnp.bfloat16)


def transform_own_samples(table, records, position, shots, slots):
    freqs, span = table[0].shape
    receivers = records.shape[1]
    rows, cols = 4 * len(slots) * shots, span * shots
    block = min(512, receivers)
    return pl.pallas_call(
        functools.partial(transform_kernel, shots=shots, slots=slots),
        grid=(receivers // block,),
        in_specs=[
            pl.BlockSpec(memory_space=pltpu.SMEM),
            pl.BlockSpec((freqs, span), lambda i: (0, 0)),
            pl.BlockSpec((freqs, span), lambda i: (0, 0)),
            pl.BlockSpec((cols, block), lambda i: (0, i)),
        ],
        out_specs=[pl.BlockSpec((rows // 4, block), lambda i: (0, i))] * 4,
        out_shape=[
            jax.ShapeDtypeStruct((rows // 4, receivers), dtype)
            for dtype in (jnp.float32, jnp.float32, jnp.bfloat16, jnp.bfloat16)
        ],
        scratch_shapes=[pltpu.VMEM((rows, cols), jnp.bfloat16)],
        name="transform_own_samples",
    )(position.reshape(1), *table, records)


def mask_green(green_rec, block_map):
    parts, receivers, points = green_rec.shape
    row_blocks, tiles = block_map.shape
    col_span = points // tiles
    col_pick = (jnp.arange(points)[None, :] // col_span == jnp.arange(tiles)[:, None]).astype(jnp.bfloat16)
    columns = jnp.dot(block_map.astype(jnp.bfloat16), col_pick, preferred_element_type=jnp.bfloat16)
    split = green_rec.reshape(parts, row_blocks, receivers // row_blocks, points)
    return (split * columns[None, :, None, :]).reshape(parts, receivers, points)


def partial_body(traces, freq_index, block_map, green_rec, green_src):
    shards = lax.axis_size("freq")
    chips = shards // 2
    span, receivers, shots = traces.shape
    points = green_rec.shape[3]
    length = span * shards
    position = lax.axis_index("freq")
    records = traces.transpose(0, 2, 1).reshape(span * shots, receivers)
    table = local_table(freq_index, length, span, position)

    def across(array, offset):
        return lax.ppermute(array, "freq", [(j, j ^ offset) for j in range(shards)])

    def chip_sums(keep, received):
        return (keep + received.astype(jnp.float32)).reshape(-1, 2 * shots, receivers)

    far = range(chips // 2, chips)
    passed = [k for k in far if k >= 3 * chips // 4 and k % 2 == 1]
    summed = [k ^ 1 for k in passed]
    straight = [k for k in reversed(far) if k < 3 * chips // 4]
    near = list(range(chips // 2))
    far_slots = passed + summed + straight

    far_keep, near_keep, far_send, near_send = transform_own_samples(
        table, records, position, shots, tuple(far_slots + near)
    )
    far_received = across(far_send, 1)
    near_received = across(near_send, 1)
    far = chip_sums(far_keep, far_received)
    cut = len(passed)
    beside = across(far[:cut].astype(jnp.bfloat16), 2)
    arrived = [
        across(far[2 * cut + i].astype(jnp.bfloat16), 2 * k) for i, k in enumerate(straight)
    ]
    far_sums = far[cut : 2 * cut] + beside.astype(jnp.float32)
    far_sums, near_received, near_keep, late_map = lax.optimization_barrier(
        (far_sums, near_received, near_keep, block_map)
    )
    arrived += [across(far_sums[i].astype(jnp.bfloat16), 2 * k) for i, k in enumerate(summed)]
    close = chip_sums(near_keep, near_received)
    arrived += [across(close[k].astype(jnp.bfloat16), 2 * k) for k in reversed(near[1:])]
    masked = mask_green(green_rec[0], late_map)
    total = close[0]
    for piece in arrived:
        total = total + piece.astype(jnp.float32)
    spectrum = (total * (1.0 / math.sqrt(length))).astype(jnp.bfloat16)
    swapped = jnp.concatenate((spectrum[shots:], -spectrum[:shots]), axis=0)
    back = jnp.dot(spectrum, masked[0], preferred_element_type=jnp.float32)
    back = back + jnp.dot(swapped, masked[1], preferred_element_type=jnp.float32)
    weights = green_src.astype(jnp.float32).reshape(2 * shots, points)
    image = jnp.sum(weights * back, axis=0)
    pieces = lax.all_to_all(
        image.reshape(shards, points // shards), "freq", split_axis=0, concat_axis=0, tiled=True
    )
    return jnp.sum(pieces, axis=0)


def body(traces, freq_index, block_map, green_rec, green_src):
    shards = lax.axis_size("freq")
    freqs = freq_index.shape[0]
    paired_chips = shards >= 8 and shards & (shards - 1) == 0
    if freqs == shards and paired_chips and 2 * freqs <= traces.shape[0]:
        return partial_body(traces, freq_index, block_map, green_rec, green_src)
    return regrouped_body(traces, freq_index, block_map, green_rec, green_src)


def solution(mesh):
    in_specs = (
        P("freq", None, "groups"),
        P(),
        P(),
        P("freq", None, None, "groups"),
        P("freq", None, None, "groups"),
    )
    out_specs = P(("groups", "freq"))
    return jax.shard_map(body, mesh=mesh, in_specs=in_specs, out_specs=out_specs, check_vma=False)
```
